128 devices in a mesh: dp: 16 (over z_lo, x, core), mp: 8 (over z_hi, y).
Axes of the slice: x: 4, y: 4, z: 4 (z_hi: 2, z_lo: 2; z = z_hi * 2 + z_lo), core: 2. Of those that a mesh axis runs over, the one named last changes fastest.
Arguments:
- tokens: bfloat16 [1024, 8192], P('mp', 'dp'), may hold values from -6 to 6
- cotangent: bfloat16 [1024, 8192], P('mp', 'dp'), may hold values from -1.5 to 1.5
- gate_weight: bfloat16 [8192, 14336], P('dp', 'mp'), may hold values from -0.0625 to 0.0625
- up_weight: bfloat16 [8192, 14336], P('dp', 'mp'), may hold values from -0.0625 to 0.0625
- down_weight: bfloat16 [14336, 8192], P('mp', 'dp'), may hold values from -0.046875 to 0.046875
Outputs:
- output: bfloat16 [1024, 8192], P('mp', 'dp')
- grad_input: bfloat16 [1024, 8192], P('mp', 'dp')
- grad_gate: bfloat16 [8192, 14336], P('dp', 'mp')
- grad_up: bfloat16 [8192, 14336], P('dp', 'mp')
- grad_down: bfloat16 [14336, 8192], P('mp', 'dp')
The draws below stay inside these ranges and needn't reach their ends.
All inputs are finite; a program needn't handle non-finite values.
Results may differ from the reference program's by a relative error of at most 0.013.
Values may be sent and summed in bfloat16 or wider, within the bound.
A program may use at most 128 MiB of HBM per device.

```python
import jax
import jax.numpy as jnp
from jax import lax

D = 8192
FF = 14336
TOKENS = 1024


def shard_levels(rng, extent, split, least, high):
    def one(position, blocks):
        steps = jax.random.uniform(jax.random.fold_in(jax.random.fold_in(rng, 6), position), (blocks,), jnp.float32, least / len(split), high / len(split))
        return jnp.repeat(jnp.exp(steps), extent[position] // blocks).reshape((-1,) + (1,) * (len(extent) - position - 1))

    factor_of = one(*split[0])
    for cut in split[1:]:
        factor_of = factor_of * one(*cut)
    return factor_of


def centred(key, shape, width, reach, shards=(), dtype=jnp.bfloat16):
    level = shard_levels(key, shape, shards, -0.22, 0.18) if shards else 1.0
    drawn = jax.random.normal(key, shape, jnp.float32) * width * level
    return jnp.minimum(jnp.maximum(drawn, -reach), reach).astype(dtype)


def setup_inputs(seed: int = 0) -> dict:
    splits = jax.random.split(jax.random.key(seed), 6)
    return {
        "tokens": centred(splits[0], (TOKENS, D), 1.0, 6.0, ((0, 8), (1, 16))),
        "cotangent": centred(splits[1], (TOKENS, D), 0.25, 1.5, ((0, 8), (1, 16))),
        "gate_weight": centred(splits[2], (D, FF), D ** -0.5, 0.0625, ((0, 16), (1, 8))),
        "up_weight": centred(splits[3], (D, FF), D ** -0.5, 0.0625, ((0, 16), (1, 8))),
        "down_weight": centred(splits[4], (FF, D), FF ** -0.5, 0.046875, ((0, 8), (1, 16))),
    }


def contract(left, right, left_dim, right_dim):
    return lax.dot_general(left, right, (((left_dim,), (right_dim,)), ((), ())), preferred_element_type=jnp.float32)


def reference(tokens, cotangent, gate_weight, up_weight, down_weight):
    gate = jnp.dot(tokens, gate_weight, preferred_element_type=jnp.float32)
    up = jnp.dot(tokens, up_weight, preferred_element_type=jnp.float32)
    sig = jax.nn.sigmoid(gate)
    hidden = (gate * sig * up).astype(jnp.bfloat16)
    output = jnp.dot(hidden, down_weight, preferred_element_type=jnp.float32).astype(jnp.bfloat16)
    d_hidden = contract(cotangent, down_weight, 1, 1)
    d_gate = (d_hidden * up * sig * (1.0 + gate * (1.0 - sig))).astype(jnp.bfloat16)
    d_up = (d_hidden * gate * sig).astype(jnp.bfloat16)
    grad_down = contract(hidden, cotangent, 0, 0).astype(jnp.bfloat16)
    grad_gate = contract(tokens, d_gate, 0, 0).astype(jnp.bfloat16)
    grad_up = contract(tokens, d_up, 0, 0).astype(jnp.bfloat16)
    grad_input = (contract(d_gate, gate_weight, 1, 1) + contract(d_up, up_weight, 1, 1)).astype(jnp.bfloat16)
    return (output, grad_input, grad_gate, grad_up, grad_down)
```

```python
import functools

import jax
import jax.numpy as jnp
from jax import lax
from jax.experimental import pallas as pl
from jax.experimental.pallas import tpu as pltpu
from jax.sharding import PartitionSpec as P

MESH = pl.DeviceIdType.MESH
F32 = jnp.float32
BF16 = jnp.bfloat16
TILE = 256


def dot(a, b, ca, cb):
    return lax.dot_general(a, b, (((ca,), (cb,)), ((), ())), preferred_element_type=F32)


def rows(start, size, step):
    return pl.ds(pl.multiple_of(start, step), size)


def kernel(
    tok, cot, wg, wu, wd,
    out, gin, gg, gu, gd,
    tc, part, cin, midl, midr, xl, xr, fo, zs, zr, hid, o, yml, ymr, yl, yr, yzs, yzr,
    send_sem, recv_sem,
):
    feat, ff = wg.shape
    wide = 3 * ff
    dp, mp = lax.axis_index("dp"), lax.axis_index("mp")
    zl, x, k = dp // 8, (dp // 2) % 4, dp % 2
    zh, y = mp // 4, mp % 4
    xp, xm, x2 = (x + 1) % 4, (x + 3) % 4, (x + 2) % 4
    yp, ym = (y + 1) % 4, (y + 3) % 4
    core = (zl * 8 + x * 2 + 1 - k, mp)
    right = (zl * 8 + xp * 2 + k, mp)
    left = (zl * 8 + xm * 2 + k, mp)
    zpeer = ((1 - zl) * 8 + x * 2 + k, mp)
    up_y = (dp, zh * 4 + yp)
    dn_y = (dp, zh * 4 + ym)
    zhpeer = (dp, (1 - zh) * 4 + y)

    barrier = pltpu.get_barrier_semaphore()
    peers = (core, right, left, zpeer, up_y, dn_y, zhpeer)
    for p in peers:
        pl.semaphore_signal(barrier, inc=1, device_id=p, device_id_type=MESH)

    sent = []
    names = {}

    def sem(name):
        return names.setdefault(name, len(names))

    def send(name, src, dst, device, index=None):
        number = len(sent)
        at = sem(name) if index is None else index
        copy = pltpu.make_async_remote_copy(
            src_ref=src, dst_ref=dst, send_sem=send_sem.at[number], recv_sem=recv_sem.at[at],
            device_id=device, device_id_type=MESH,
        )
        copy.start()
        sent.append(copy)

    def recv(name, ref, index=None):
        at = sem(name) if index is None else index
        pltpu.make_async_remote_copy(
            src_ref=ref, dst_ref=ref, send_sem=send_sem.at[0], recv_sem=recv_sem.at[at],
            device_id=core, device_id_type=MESH,
        ).wait_recv()

    s10 = sem("s1a"); sem("s1b")
    s20 = sem("s2a"); sem("s2b")

    def block(slot, half):
        return tc.at[rows(slot * 256 + half * 128, 128, 128)]

    own = rows(zh * 128, 128, 128)
    tc[own, :feat] = tok[...]
    tc[own, feat:] = cot[...]
    pl.semaphore_wait(barrier, len(peers))
    send("z0", block(0, zh), block(0, zh), zhpeer)
    send("", block(0, zh), block(1, zh), dn_y, s10 + zh)
    send("", block(0, zh), block(2, zh), up_y, s20 + zh)

    def gather0():
        recv("z0", block(0, 1 - zh))
        send("", block(0, 1 - zh), block(1, 1 - zh), dn_y, s10 + 1 - zh)
        send("", block(0, 1 - zh), block(2, 1 - zh), up_y, s20 + 1 - zh)

    def gather1():
        recv("", block(1, 0), s10)
        send("s3a", block(1, 0), block(3, 0), dn_y)
        recv("", block(2, 1), s20 + 1)
        send("s3b", block(2, 1), block(3, 1), up_y)
        recv("", block(1, 1), s10 + 1)

    def gather2():
        recv("", block(2, 0), s20)

    def gather3():
        recv("s3a", block(3, 0))
        recv("s3b", block(3, 1))

    def first(s):
        @pl.loop(0, ff // TILE)
        def _(n):
            here = rows(s * 256, 256, 256)
            c = rows(n * TILE, TILE, TILE)
            t = tc[here, :feat]
            part[here, c] = dot(t, wg[:, c], 1, 0).astype(BF16)
            part[here, rows(ff + n * TILE, TILE, TILE)] = dot(t, wu[:, c], 1, 0).astype(BF16)
            part[here, rows(2 * ff + n * TILE, TILE, TILE)] = dot(
                tc[here, feat:], wd[c, :], 1, 1
            ).astype(BF16)

        send(f"c{s}", part.at[rows(s * 256 + (1 - k) * 128, 128, 128)], cin.at[s], core)

    def piece(s, xx, half):
        return rows(s * 256 + k * 128 + xx * 32 + half * 16, 16, 16)

    def core_sum(s, xx):
        @pl.loop(0, 2)
        def _(h):
            r = piece(s, xx, h)
            other = rows(xx * 32 + h * 16, 16, 16)
            for j in range(3):
                c = slice(j * ff, (j + 1) * ff)
                part[r, c] = (part[r, c].astype(F32) + cin[s, other, c].astype(F32)).astype(BF16)

    lo, hi = slice(0, 16), slice(16, 32)

    def sum1(s):
        recv(f"c{s}", cin.at[s])
        core_sum(s, x2)
        send(f"ml{s}", part.at[piece(s, x2, 0)], midl.at[s], right)
        send(f"mr{s}", part.at[piece(s, x2, 1)], midr.at[s], left)
        core_sum(s, xp)
        send(f"xlh{s}", part.at[piece(s, xp, 1)], xl.at[s, hi], right)
        core_sum(s, xm)
        send(f"xrl{s}", part.at[piece(s, xm, 0)], xr.at[s, lo], left)
        core_sum(s, x)

    def add_to(ref, r, c, other):
        ref[r, c] = (ref[r, c].astype(F32) + other.astype(F32)).astype(BF16)

    def sum2(s):
        recv(f"ml{s}", midl.at[s])
        for j in range(3):
            c = slice(j * ff, (j + 1) * ff)
            add_to(part, piece(s, xp, 0), c, midl[s, :, c])
        send(f"xll{s}", part.at[piece(s, xp, 0)], xl.at[s, lo], right)
        recv(f"mr{s}", midr.at[s])
        for j in range(3):
            c = slice(j * ff, (j + 1) * ff)
            add_to(part, piece(s, xm, 1), c, midr[s, :, c])
        send(f"xrh{s}", part.at[piece(s, xm, 1)], xr.at[s, hi], left)

    def sum3(s):
        recv(f"xlh{s}", xl.at[s, hi])
        recv(f"xrl{s}", xr.at[s, lo])
        recv(f"xll{s}", xl.at[s, lo])
        recv(f"xrh{s}", xr.at[s, hi])
        mine, theirs = rows(zl * 16, 16, 16), rows((1 - zl) * 16, 16, 16)
        for j in range(3):
            c = slice(j * ff, (j + 1) * ff)
            zs[s, :, c] = (
                part[piece(s, x, 1 - zl), c].astype(F32)
                + xl[s, theirs, c].astype(F32)
                + xr[s, theirs, c].astype(F32)
            ).astype(BF16)
        send(f"z{s}", zs.at[s], zr.at[s], zpeer, sem(f"zz{s}"))
        for j in range(3):
            c = slice(j * ff, (j + 1) * ff)
            fo[s, :, c] = (
                part[piece(s, x, zl), c].astype(F32)
                + xl[s, mine, c].astype(F32)
                + xr[s, mine, c].astype(F32)
            )

    def middle(s):
        recv(f"zz{s}", zr.at[s])
        r = piece(s, x, zl)

        @pl.loop(0, ff // TILE)
        def _(n):
            def value(j):
                c = rows(j * ff + n * TILE, TILE, TILE)
                return fo[s, :, c] + zr[s, :, c].astype(F32)

            gate, up, dh = value(0), value(1), value(2)
            sig = 1.0 / (1.0 + jnp.exp(-gate))
            act = gate * sig
            hid[r, rows(n * TILE, TILE, TILE)] = (act * up).astype(BF16)
            hid[r, rows(ff + n * TILE, TILE, TILE)] = (
                dh * up * sig * (1.0 + gate * (1.0 - sig))
            ).astype(BF16)
            hid[r, rows(2 * ff + n * TILE, TILE, TILE)] = (dh * act).astype(BF16)

    def forward(name, r, device, index=None):
        send(name, hid.at[r], hid.at[r], device, index)

    def spread1(s):
        l0 = sem(f"gl{s}0"); sem(f"gl{s}1")
        r0 = sem(f"gr{s}0"); sem(f"gr{s}1")
        r = piece(s, x, zl)
        forward("", r, right, l0 + zl)
        forward("", r, left, r0 + zl)
        forward(f"gz{s}", r, zpeer)

    def pair(s, xx):
        return rows(s * 256 + k * 128 + xx * 32, 32, 32)

    def spread2(s):
        l0, r0 = sem(f"gl{s}0"), sem(f"gr{s}0")
        r = piece(s, x, 1 - zl)
        recv(f"gz{s}", hid.at[r])
        forward("", r, right, l0 + 1 - zl)
        forward("", r, left, r0 + 1 - zl)
        forward(f"gc{s}0", pair(s, x), core)

    def spread3(s):
        l0, r0 = sem(f"gl{s}0"), sem(f"gr{s}0")
        recv("", hid.at[piece(s, xm, 0)], l0)
        forward(f"fl{s}", piece(s, xm, 0), right)
        recv("", hid.at[piece(s, xp, 1)], r0 + 1)
        forward(f"fr{s}", piece(s, xp, 1), left)
        recv("", hid.at[piece(s, xm, 1)], l0 + 1)
        forward(f"gc{s}1", pair(s, xm), core)
        recv("", hid.at[piece(s, xp, 0)], r0)
        forward(f"gc{s}2", pair(s, xp), core)

    def spread4(s):
        recv(f"fl{s}", hid.at[piece(s, x2, 0)])
        recv(f"fr{s}", hid.at[piece(s, x2, 1)])
        forward(f"gc{s}3", pair(s, x2), core)

    def last(s):
        for i, xx in enumerate((x, xm, xp, x2)):
            other = rows(s * 256 + (1 - k) * 128 + xx * 32, 32, 32)
            recv(f"gc{s}{i}", hid.at[other])
        here = rows(s * 256, 256, 256)

        @pl.loop(0, feat // TILE)
        def _(n):
            c = rows(n * TILE, TILE, TILE)
            o[here, c] = dot(hid[here, :ff], wd[:, c], 1, 0).astype(BF16)
            o[here, rows(feat + n * TILE, TILE, TILE)] = (
                dot(hid[here, ff : 2 * ff], wg[c, :], 1, 1) + dot(hid[here, 2 * ff :], wu[c, :], 1, 1)
            ).astype(BF16)

    def oblock(s, half):
        return o.at[slice(s * 256 + half * 128, s * 256 + half * 128 + 128)]

    def out3():
        send("yml", oblock(3, 0), yml, up_y)
        send("ymr", oblock(3, 1), ymr, dn_y)

    def out1():
        send("ylh", oblock(1, 1), yl.at[128:256], up_y)

    def out1b():
        recv("yml", yml)
        o[256:384] = (o[256:384].astype(F32) + yml[...].astype(F32)).astype(BF16)
        send("yll", oblock(1, 0), yl.at[0:128], up_y)

    def out2():
        send("yrl", oblock(2, 0), yr.at[0:128], dn_y)
        recv("ymr", ymr)
        o[640:768] = (o[640:768].astype(F32) + ymr[...].astype(F32)).astype(BF16)
        send("yrh", oblock(2, 1), yr.at[128:256], dn_y)

    def out0():
        recv("ylh", yl.at[128:256])
        recv("yll", yl.at[0:128])
        recv("yrl", yr.at[0:128])
        recv("yrh", yr.at[128:256])
        theirs = rows((1 - zh) * 128, 128, 128)
        yzs[...] = (
            o[theirs].astype(F32) + yl[theirs].astype(F32) + yr[theirs].astype(F32)
        ).astype(BF16)
        send("yz", yzs, yzr, zhpeer)

    def out0b():
        recv("yz", yzr)
        mine = rows(zh * 128, 128, 128)
        total = (
            o[mine].astype(F32) + yl[mine].astype(F32) + yr[mine].astype(F32)
            + yzr[...].astype(F32)
        )
        out[...] = total[:, :feat].astype(BF16)
        gin[...] = total[:, feat:].astype(BF16)

    def grads():
        @pl.loop(0, ff // TILE)
        def _(n):
            c = rows(n * TILE, TILE, TILE)
            gd[c, :] = dot(hid[:, c], tc[:, feat:], 0, 0).astype(BF16)
            gg[:, c] = dot(tc[:, :feat], hid[:, rows(ff + n * TILE, TILE, TILE)], 0, 0).astype(BF16)
            gu[:, c] = dot(
                tc[:, :feat], hid[:, rows(2 * ff + n * TILE, TILE, TILE)], 0, 0
            ).astype(BF16)

    gather0()
    first(0)
    gather1()
    first(1)
    sum1(0)
    gather2()
    first(2)
    sum1(1)
    sum2(0)
    gather3()
    first(3)
    sum1(2)
    sum2(1)
    sum3(0)
    sum1(3)
    sum2(2)
    sum3(1)
    sum2(3)
    middle(1)
    spread1(1)
    sum3(2)
    spread2(1)
    sum3(3)
    middle(3)
    spread1(3)
    middle(2)
    spread3(1)
    spread2(3)
    spread1(2)
    spread4(1)
    spread3(3)
    spread2(2)
    middle(0)
    spread1(0)
    last(1)
    out1()
    spread4(3)
    spread3(2)
    spread2(0)
    last(3)
    out3()
    spread4(2)
    spread3(0)
    out1b()
    last(2)
    out2()
    spread4(0)
    last(0)
    out0()
    grads()
    out0b()
    for copy in sent:
        copy.wait_send()


def per_device(tokens, cotangent, gate_weight, up_weight, down_weight):
    n, feat = tokens.shape
    ff = gate_weight.shape[1]
    wide = 3 * ff
    vmem = pl.BlockSpec(memory_space=pltpu.VMEM)
    shape = lambda a: jax.ShapeDtypeStruct(a.shape, BF16)
    buf = lambda *s: pltpu.VMEM(s, BF16)
    return pl.pallas_call(
        kernel,
        out_shape=tuple(shape(a) for a in (tokens, cotangent, gate_weight, up_weight, down_weight)),
        in_specs=[vmem] * 5,
        out_specs=[vmem] * 5,
        scratch_shapes=[
            buf(1024, 2 * feat),
            buf(1024, wide),
            buf(4, 128, wide),
            buf(4, 16, wide),
            buf(4, 16, wide),
            buf(4, 32, wide),
            buf(4, 32, wide),
            pltpu.VMEM((4, 16, wide), F32),
            buf(4, 16, wide),
            buf(4, 16, wide),
            buf(1024, wide),
            buf(1024, 2 * feat),
            buf(128, 2 * feat),
            buf(128, 2 * feat),
            buf(256, 2 * feat),
            buf(256, 2 * feat),
            buf(128, 2 * feat),
            buf(128, 2 * feat),
            pltpu.SemaphoreType.DMA((160,)),
            pltpu.SemaphoreType.DMA((160,)),
        ],
        compiler_params=pltpu.CompilerParams(
            collective_id=0, has_side_effects=True, vmem_limit_bytes=67043328
        ),
    )(tokens, cotangent, gate_weight, up_weight, down_weight)


def solution(mesh):
    placed = (P("mp", "dp"), P("mp", "dp"), P("dp", "mp"), P("dp", "mp"), P("mp", "dp"))
    return jax.shard_map(
        per_device, mesh=mesh, in_specs=placed, out_specs=placed, check_vma=False
    )
```

```python
import jax
import jax.numpy as jnp
from jax import lax
from jax.experimental import pallas as pl
from jax.experimental.pallas import tpu as pltpu
from jax.sharding import PartitionSpec as P

MESH = pl.DeviceIdType.MESH
F32 = jnp.float32
BF16 = jnp.bfloat16
ROWS = 128

CHUNKS = ((3, 0), (2, 1), (1, 1), (0, 1), (3, 1), (1, 0), (2, 0), (0, 0))
NUMBER = {c: i for i, c in enumerate(CHUNKS)}
EARLY = 4
ORDER = (
    ("start",), ("first", 7), ("sum1", 7), ("gb", 0), ("first", 5), ("gb2", 0), ("sum2a", 7), ("sum2b", 7),
    ("ga",), ("first", 6), ("sum2c", 7), ("first", 3), ("sum1", 5), ("sum1", 6), ("gc", 0), ("first", 0),
    ("sum1", 3), ("sum2c", 5), ("gb", 1), ("sum2a", 5), ("first", 2), ("gb2", 1), ("sum1", 0), ("sum2b", 6),
    ("first", 1), ("sum3a", 7), ("sum1", 2), ("gc", 1), ("sum2a", 6), ("sum2b", 5), ("sum1", 1), ("first", 4),
    ("sum2b", 0), ("sum2a", 0), ("sum2c", 0), ("sum3a", 6), ("sum2a", 1), ("sum2c", 1), ("sum1", 4),
    ("sum3a", 5), ("sum3b", 0), ("sum3b", 1), ("sum2b", 1), ("sum2a", 2), ("sum2b", 3), ("sum3a", 0),
    ("sum2b", 4), ("sum2c", 4), ("sum2a", 4), ("sum3b", 5), ("sum2a", 3), ("sum2c", 3), ("sum2c", 6),
    ("sum3a", 1), ("sum2b", 2), ("middle", 0), ("sum2c", 2), ("sum3a", 4), ("middle", 1), ("sum3a", 2),
    ("sum3b", 4), ("s1", 0), ("sum3b", 2), ("s2a", 0), ("s1", 1), ("sum3b", 6), ("s2a", 1), ("middle", 4),
    ("middle", 2), ("s3", 0), ("s2b", 0), ("sum3b", 7), ("s1", 4), ("sum3a", 3), ("sum3b", 3), ("s2a", 4),
    ("middle", 6), ("s1", 2), ("s2b", 4), ("s2a", 2), ("s3", 1), ("s3", 4), ("s2b", 1), ("middle", 3),
    ("s4", 0), ("s2a", 6), ("s1", 6), ("s2b", 2), ("middle", 5), ("s4", 4), ("s3", 2), ("s4", 1), ("last", 0),
    ("s1", 3), ("s2a", 3), ("out", 3, 0), ("s3", 6), ("last", 4), ("s2b", 6), ("out", 3, 1), ("s1", 5),
    ("s4", 2), ("last", 1), ("s2a", 5), ("s2b", 3), ("s3", 3), ("middle", 7), ("s4", 6), ("out", 2, 1),
    ("last", 2), ("s2b", 5), ("relay", 1, 1), ("s3", 5), ("out", 1, 1), ("relay", 2, 1), ("s4", 3), ("s1", 7),
    ("last", 6), ("relay", 2, 0), ("s2a", 7), ("out", 2, 0), ("s4", 5), ("last", 3), ("grad", 0), ("s3", 7),
    ("s2b", 7), ("last", 5), ("fin1",), ("relay", 1, 0), ("grad", 1), ("out", 1, 0), ("s4", 7), ("grad", 2),
    ("grad", 3), ("grad", 4), ("grad", 5), ("last", 7), ("fin0",),
)


def dot(a, b, ca, cb):
    return lax.dot_general(a, b, (((ca,), (cb,)), ((), ())), preferred_element_type=F32)


def at_rows(start, size, step):
    return pl.ds(pl.multiple_of(start, step), size)


def exchange(
    tok, cot, wg_hbm, wu_hbm, wd_hbm,
    both, gg_hbm, gu_hbm, gd_hbm, late, tclate,
    tc, wg, wu, wd, part, cin, midl, midr, xl, xr, fo, zs, zr, zd, dmid, dxl, dxr, hid,
    o, yml, ymr, yl, yr, yzs, yzr, gg, gu, gd,
    send_sem, recv_sem, copy_sem,
):
    feat, ff = wg.shape
    half = ff // 2
    gu_cols, dh_cols = slice(0, 2 * half), slice(2 * half, 3 * half)
    dp, mp = lax.axis_index("dp"), lax.axis_index("mp")
    zl, x, k = dp // 8, (dp // 2) % 4, dp % 2
    zh, y = mp // 4, mp % 4
    xp, xm, x2 = (x + 1) % 4, (x + 3) % 4, (x + 2) % 4
    core = (zl * 8 + x * 2 + 1 - k, mp)
    right = (zl * 8 + xp * 2 + k, mp)
    left = (zl * 8 + xm * 2 + k, mp)
    zpeer = ((1 - zl) * 8 + x * 2 + k, mp)
    up_y = (dp, zh * 4 + (y + 1) % 4)
    dn_y = (dp, zh * 4 + (y + 3) % 4)
    zhpeer = (dp, (1 - zh) * 4 + y)

    local = []

    def fetch(src, dst):
        copy = pltpu.make_async_copy(src, dst, copy_sem.at[len(local)])
        copy.start()
        local.append(copy)
        return copy

    weights = [fetch(wg_hbm, wg), fetch(wu_hbm, wu), fetch(wd_hbm, wd)]
    barrier = pltpu.get_barrier_semaphore()
    peers = (core, right, left, zpeer, up_y, dn_y, zhpeer)
    for p in peers:
        pl.semaphore_signal(barrier, inc=1, device_id=p, device_id_type=MESH)

    sent = []
    names = {}

    def sem(name):
        return names.setdefault(name, len(names))

    def send(name, src, dst, device, index=None):
        at = sem(name) if index is None else index
        copy = pltpu.make_async_remote_copy(
            src_ref=src, dst_ref=dst, send_sem=send_sem.at[len(sent)], recv_sem=recv_sem.at[at],
            device_id=device, device_id_type=MESH,
        )
        copy.start()
        sent.append(copy)

    def recv(name, ref, index=None):
        at = sem(name) if index is None else index
        pltpu.make_async_remote_copy(
            src_ref=ref, dst_ref=ref, send_sem=send_sem.at[0], recv_sem=recv_sem.at[at],
            device_id=core, device_id_type=MESH,
        ).wait_recv()

    def chunk(c):
        return slice(c * ROWS, (c + 1) * ROWS)

    def tokens(slot, rel, piece=slice(0, ROWS)):
        base = NUMBER[slot, rel] * ROWS
        return tc.at[base + piece.start : base + piece.stop]

    lo, hi = slice(0, ROWS // 2), slice(ROWS // 2, ROWS)

    def start():
        own = chunk(NUMBER[0, 0])
        tc[own, :feat] = tok[...]
        tc[own, feat:] = cot[...]
        pl.semaphore_wait(barrier, len(peers))
        send("t01", tokens(0, 0), tokens(0, 1), zhpeer)
        send("t10", tokens(0, 0), tokens(1, 0), dn_y)
        send("t20", tokens(0, 0), tokens(2, 0), up_y)
        for copy in weights:
            copy.wait()

    def gather_a():
        recv("t01", tokens(0, 1))
        send("t11", tokens(0, 1), tokens(1, 1), dn_y)
        send("t21", tokens(0, 1), tokens(2, 1), up_y)

    def gather_b(rel):
        recv(f"t1{rel}", tokens(1, rel))
        send(f"t3{rel}a", tokens(1, rel, lo), tokens(3, rel, lo), dn_y)

    def gather_b2(rel):
        recv(f"t2{rel}", tokens(2, rel))
        send(f"t3{rel}b", tokens(2, rel, hi), tokens(3, rel, hi), up_y)

    def gather_c(rel):
        recv(f"t3{rel}a", tokens(3, rel, lo))
        recv(f"t3{rel}b", tokens(3, rel, hi))

    def first(c):
        here = chunk(c)

        @pl.loop(0, 2)
        def _(q):
            c0 = at_rows(q * half, half, 128)
            part[q, here, :half] = dot(tc[here, :feat], wg[:, c0], 1, 0).astype(BF16)
            part[q, here, half : 2 * half] = dot(tc[here, :feat], wu[:, c0], 1, 0).astype(BF16)
            part[q, here, 2 * half :] = dot(tc[here, feat:], wd[c0, :], 1, 1).astype(BF16)

        send(f"c{c}", part.at[1 - k, here], cin.at[c], core)

    def piece(c, xx, zz):
        return at_rows(c * ROWS + zz * 64 + xx * 16, 16, 16)

    thirds = [slice(j * half, (j + 1) * half) for j in range(3)]

    def add_to(r, cols, other):
        part[k, r, cols] = (part[k, r, cols].astype(F32) + other.astype(F32)).astype(BF16)

    def core_sum(c, xx, zz):
        for cols in thirds[:2]:
            add_to(piece(c, xx, zz), cols, cin[c, at_rows(zz * 64 + xx * 16, 16, 16), cols])

    def core_sum_dh(c, zz):
        @pl.loop(0, 4)
        def _(i):
            add_to(piece(c, i, zz), dh_cols, cin[c, at_rows(zz * 64 + i * 16, 16, 16), dh_cols])

    def gu_part(r):
        return part.at[k, r, gu_cols]

    def dh_part(r):
        return part.at[k, r, dh_cols]

    def sum1(c):
        recv(f"c{c}", cin.at[c])
        core_sum(c, x2, 0)
        send(f"ml{c}", gu_part(piece(c, x2, 0)), midl.at[c], right)
        core_sum(c, x2, 1)
        send(f"mr{c}", gu_part(piece(c, x2, 1)), midr.at[c], left)
        core_sum_dh(c, 1 - zl)
        send(f"zd{c}", dh_part(at_rows(c * ROWS + (1 - zl) * 64, 64, 64)), zd.at[c], zpeer)
        core_sum(c, xp, 1)
        send(f"xl{c}1", gu_part(piece(c, xp, 1)), xl.at[c, 1], right)
        core_sum(c, xm, 0)
        send(f"xr{c}0", gu_part(piece(c, xm, 0)), xr.at[c, 0], left)
        core_sum(c, xp, 0)
        core_sum(c, xm, 1)
        core_sum(c, x, 0)
        core_sum(c, x, 1)
        core_sum_dh(c, zl)

    def sum2a(c):
        recv(f"ml{c}", midl.at[c])
        for cols in thirds[:2]:
            add_to(piece(c, xp, 0), cols, midl[c, :, cols])
        send(f"xl{c}0", gu_part(piece(c, xp, 0)), xl.at[c, 0], right)

    def sum2b(c):
        recv(f"mr{c}", midr.at[c])
        for cols in thirds[:2]:
            add_to(piece(c, xm, 1), cols, midr[c, :, cols])
        send(f"xr{c}1", gu_part(piece(c, xm, 1)), xr.at[c, 1], left)

    def sum2c(c):
        recv(f"zd{c}", zd.at[c])

        def add_dh(xx):
            add_to(piece(c, xx, zl), dh_cols, zd[c, at_rows(xx * 16, 16, 16), :])

        add_dh(x2)
        far = dh_part(piece(c, x2, zl))
        if c % 2:
            send(f"dm{c}", far, dmid.at[c], left)
            add_dh(xp)
            send(f"dl{c}", dh_part(piece(c, xp, zl)), dxl.at[c], right)
            add_dh(xm)
        else:
            send(f"dm{c}", far, dmid.at[c], right)
            add_dh(xm)
            send(f"dr{c}", dh_part(piece(c, xm, zl)), dxr.at[c], left)
            add_dh(xp)
        add_dh(x)

    def sum3a(c):
        recv(f"xl{c}1", xl.at[c, 1])
        recv(f"xr{c}0", xr.at[c, 0])
        recv(f"xl{c}0", xl.at[c, 0])
        recv(f"xr{c}1", xr.at[c, 1])
        for cols in thirds[:2]:
            zs[c, :, cols] = (
                part[k, piece(c, x, 1 - zl), cols].astype(F32)
                + xl[c, 1 - zl, :, cols].astype(F32)
                + xr[c, 1 - zl, :, cols].astype(F32)
            ).astype(BF16)
        send(f"zz{c}", zs.at[c], zr.at[c], zpeer)
        for cols in thirds[:2]:
            fo[c, :, cols] = (
                part[k, piece(c, x, zl), cols].astype(F32)
                + xl[c, zl, :, cols].astype(F32)
                + xr[c, zl, :, cols].astype(F32)
            )

    def sum3b(c):
        recv(f"dm{c}", dmid.at[c])
        if c % 2:
            add_to(piece(c, xm, zl), dh_cols, dmid[c])
            send(f"dr{c}", dh_part(piece(c, xm, zl)), dxr.at[c], left)
        else:
            add_to(piece(c, xp, zl), dh_cols, dmid[c])
            send(f"dl{c}", dh_part(piece(c, xp, zl)), dxl.at[c], right)

    def middle(c):
        recv(f"zz{c}", zr.at[c])
        recv(f"dl{c}", dxl.at[c])
        recv(f"dr{c}", dxr.at[c])
        r = piece(c, x, zl)

        @pl.loop(0, half // 128)
        def _(n):
            c0, c1, c2 = (at_rows(j * half + n * 128, 128, 128) for j in range(3))
            gate = fo[c, :, c0] + zr[c, :, c0].astype(F32)
            up = fo[c, :, c1] + zr[c, :, c1].astype(F32)
            dh = part[k, r, c2].astype(F32) + dxl[c, :, c0].astype(F32) + dxr[c, :, c0].astype(F32)
            sig = 1.0 / (1.0 + jnp.exp(-gate))
            act = gate * sig
            hid[k, r, c0] = (act * up).astype(BF16)
            hid[k, r, c1] = (dh * up * sig * (1.0 + gate * (1.0 - sig))).astype(BF16)
            hid[k, r, c2] = (dh * act).astype(BF16)

        full = hid.at[k, r]
        send("", full, full, right, sem(f"gl{c}") + zl)
        sem(f"gl{c}b")
        send("", full, full, left, sem(f"gr{c}") + zl)
        sem(f"gr{c}b")
        send(f"gz{c}", full, full, zpeer)

    def pass_on(name, r, cols, device, index=None):
        ref = hid.at[k, r, cols]
        send(name, ref, ref, device, index)

    def spread1(c):
        gl, gr = sem(f"gl{c}"), sem(f"gr{c}")
        other = piece(c, x, 1 - zl)
        recv(f"gz{c}", hid.at[k, other])
        pass_on("", other, gu_cols, right, gl + 1 - zl)
        pass_on("", other, gu_cols, left, gr + 1 - zl)

    def spread2a(c):
        gl, gr = sem(f"gl{c}"), sem(f"gr{c}")
        recv("", hid.at[k, piece(c, xm, zl)], gl + zl)
        recv("", hid.at[k, piece(c, xp, zl)], gr + zl)
        if c % 2:
            pass_on(f"fd{c}", piece(c, xp, zl), dh_cols, left)
        else:
            pass_on(f"fd{c}", piece(c, xm, zl), dh_cols, right)
        pass_on(f"du{c}m", piece(c, xm, zl), dh_cols, zpeer)
        pass_on(f"du{c}p", piece(c, xp, zl), dh_cols, zpeer)

    def spread2b(c):
        gl, gr = sem(f"gl{c}"), sem(f"gr{c}")
        recv("", hid.at[k, piece(c, xm, 1 - zl), gu_cols], gl + 1 - zl)
        recv("", hid.at[k, piece(c, xp, 1 - zl), gu_cols], gr + 1 - zl)
        pass_on(f"fl{c}", piece(c, xm, 0), gu_cols, right)
        pass_on(f"fr{c}", piece(c, xp, 1), gu_cols, left)

    def spread3(c):
        recv(f"fd{c}", hid.at[k, piece(c, x2, zl), dh_cols])
        pass_on(f"du{c}f", piece(c, x2, zl), dh_cols, zpeer)

    def spread4(c):
        recv(f"fl{c}", hid.at[k, piece(c, x2, 0), gu_cols])
        recv(f"fr{c}", hid.at[k, piece(c, x2, 1), gu_cols])
        recv(f"du{c}m", hid.at[k, piece(c, xm, 1 - zl), dh_cols])
        recv(f"du{c}p", hid.at[k, piece(c, xp, 1 - zl), dh_cols])
        recv(f"du{c}f", hid.at[k, piece(c, x2, 1 - zl), dh_cols])
        send(f"gc{c}", hid.at[k, chunk(c)], hid.at[k, chunk(c)], core)

    def last(c):
        recv(f"gc{c}", hid.at[1 - k, chunk(c)])
        here = chunk(c)
        if c >= EARLY:
            r = slice((c - EARLY) * ROWS, (c - EARLY + 1) * ROWS)
            fetch(tc.at[here], tclate.at[r])
            for q in range(2):
                for j in range(3):
                    fetch(hid.at[q, here, thirds[j]], late.at[j, r, q * half : (q + 1) * half])
        o[here, :feat] = (
            dot(hid[0, here, :half], wd[:half, :], 1, 0) + dot(hid[1, here, :half], wd[half:, :], 1, 0)
        ).astype(BF16)
        total = None
        for q in range(2):
            for j, w in ((1, wg), (2, wu)):
                term = dot(hid[q, here, thirds[j]], w[:, q * half : (q + 1) * half], 1, 1)
                total = term if total is None else total + term
        o[here, feat:] = total.astype(BF16)

    def out_rows(slot, rel, piece):
        base = NUMBER[slot, rel] * ROWS
        return slice(base + piece.start, base + piece.stop)

    def send_out(name, slot, rel, piece, dst, device):
        send(name, o.at[out_rows(slot, rel, piece)], dst, device)

    def add_out(slot, rel, piece, other):
        r = out_rows(slot, rel, piece)
        o[r] = (o[r].astype(F32) + other.astype(F32)).astype(BF16)

    def out(slot, rel):
        if slot == 3:
            send_out(f"ym{rel}l", 3, rel, lo, yml.at[rel], up_y)
            send_out(f"ym{rel}r", 3, rel, hi, ymr.at[rel], dn_y)
        if slot == 1:
            send_out(f"yl{rel}h", 1, rel, hi, yl.at[rel, hi], up_y)
        if slot == 2:
            send_out(f"yr{rel}l", 2, rel, lo, yr.at[rel, lo], dn_y)

    def relay(slot, rel):
        if slot == 1:
            recv(f"ym{rel}l", yml.at[rel])
            add_out(1, rel, lo, yml[rel])
            send_out(f"yl{rel}l", 1, rel, lo, yl.at[rel, lo], up_y)
        else:
            recv(f"ym{rel}r", ymr.at[rel])
            add_out(2, rel, hi, ymr[rel])
            send_out(f"yr{rel}h", 2, rel, hi, yr.at[rel, hi], dn_y)

    def gather_out(rel):
        recv(f"yl{rel}h", yl.at[rel, hi])
        recv(f"yr{rel}l", yr.at[rel, lo])
        recv(f"yl{rel}l", yl.at[rel, lo])
        recv(f"yr{rel}h", yr.at[rel, hi])
        r = chunk(NUMBER[0, rel])
        return o[r].astype(F32) + yl[rel].astype(F32) + yr[rel].astype(F32)

    def finish1():
        yzs[...] = gather_out(1).astype(BF16)
        send("yz", yzs, yzr, zhpeer)

    def finish0():
        total = gather_out(0)
        recv("yz", yzr)
        both[...] = (total + yzr[...].astype(F32)).astype(BF16)

    rows_early = slice(0, EARLY * ROWS)

    def grad(i):
        if i < 4:
            q, m = i // 2, i % 2
            c = slice(q * half, (q + 1) * half)
            f = slice(m * feat // 2, (m + 1) * feat // 2)
            a = tc[rows_early, f]
            gg[f, c] = dot(a, hid[q, rows_early, thirds[1]], 0, 0).astype(BF16)
            gu[f, c] = dot(a, hid[q, rows_early, thirds[2]], 0, 0).astype(BF16)
        else:
            q = i - 4

            @pl.loop(0, half // 128)
            def _(n):
                h = hid[q, rows_early, at_rows(n * 128, 128, 128)]
                gd[at_rows(q * half + n * 128, 128, 128), :] = dot(
                    h, tc[rows_early, feat:], 0, 0
                ).astype(BF16)
        if i == 3:
            fetch(gg, gg_hbm)
            fetch(gu, gu_hbm)
        if i == 5:
            fetch(gd, gd_hbm)

    steps = dict(
        start=start, ga=gather_a, gb=gather_b, gb2=gather_b2, gc=gather_c, first=first, sum1=sum1, sum2a=sum2a, sum2b=sum2b,
        sum2c=sum2c, sum3a=sum3a, sum3b=sum3b, middle=middle, s1=spread1, s2a=spread2a, s2b=spread2b, s3=spread3, s4=spread4, last=last, out=out, relay=relay,
        fin1=finish1, fin0=finish0, grad=grad,
    )
    for name, *numbers in ORDER:
        steps[name](*numbers)
    for copy in sent:
        copy.wait_send()
    for copy in local[3:]:
        copy.wait()


def finish(both, gg_in, gu_in, gd_in, h, dg, du, tc, out, gin, gg, gu, gd, turned):
    feat = out.shape[1]

    @pl.when(pl.program_id(0) == 0)
    def _():
        turned[...] = tc[:, :feat].T
        out[...] = both[:, :feat]
        gin[...] = both[:, feat:]

    t = turned[...]
    gg[...] = (gg_in[...].astype(F32) + dot(t, dg[...], 1, 0)).astype(BF16)
    gu[...] = (gu_in[...].astype(F32) + dot(t, du[...], 1, 0)).astype(BF16)
    gd[...] = (gd_in[...].astype(F32) + dot(h[...], tc[:, feat:], 0, 0)).astype(BF16)


def per_device(tokens, cotangent, gate_weight, up_weight, down_weight):
    feat, ff = gate_weight.shape
    half = ff // 2
    late = (8 - EARLY) * ROWS
    vmem = pl.BlockSpec(memory_space=pltpu.VMEM)
    hbm = pl.BlockSpec(memory_space=pl.ANY)
    shape = lambda *s: jax.ShapeDtypeStruct(s, BF16)
    buf = lambda *s: pltpu.VMEM(s, BF16)
    both, gg, gu, gd, hid, tc = pl.pallas_call(
        exchange,
        out_shape=(
            shape(ROWS, 2 * feat), shape(feat, ff), shape(feat, ff), shape(ff, feat),
            shape(3, late, ff), shape(late, 2 * feat),
        ),
        in_specs=[vmem, vmem, hbm, hbm, hbm],
        out_specs=[vmem, hbm, hbm, hbm, hbm, hbm],
        scratch_shapes=[
            buf(1024, 2 * feat), buf(feat, ff), buf(feat, ff), buf(ff, feat),
            buf(2, 1024, 3 * half), buf(8, ROWS, 3 * half),
            buf(8, 16, 2 * half), buf(8, 16, 2 * half),
            buf(8, 2, 16, 2 * half), buf(8, 2, 16, 2 * half),
            pltpu.VMEM((8, 16, 2 * half), F32), buf(8, 16, 2 * half), buf(8, 16, 2 * half),
            buf(8, 64, half), buf(8, 16, half), buf(8, 16, half), buf(8, 16, half),
            buf(2, 1024, 3 * half), buf(1024, 2 * feat),
            buf(2, 64, 2 * feat), buf(2, 64, 2 * feat),
            buf(2, ROWS, 2 * feat), buf(2, ROWS, 2 * feat),
            buf(ROWS, 2 * feat), buf(ROWS, 2 * feat),
            buf(feat, ff), buf(feat, ff), buf(ff, feat),
            pltpu.SemaphoreType.DMA((256,)), pltpu.SemaphoreType.DMA((256,)), pltpu.SemaphoreType.DMA((48,)),
        ],
        compiler_params=pltpu.CompilerParams(
            collective_id=0, has_side_effects=True, vmem_limit_bytes=67043328
        ),
    )(tokens, cotangent, gate_weight, up_weight, down_weight)
    tile = 256
    cols = pl.BlockSpec((feat, tile), lambda n: (0, n))
    down = pl.BlockSpec((tile, feat), lambda n: (n, 0))
    whole = lambda r, c: pl.BlockSpec((r, c), lambda n: (0, 0))
    third = lambda j: pl.BlockSpec((None, late, tile), lambda n: (j, 0, n))
    return pl.pallas_call(
        finish,
        grid=(ff // tile,),
        out_shape=(shape(ROWS, feat), shape(ROWS, feat), shape(feat, ff), shape(feat, ff), shape(ff, feat)),
        in_specs=[whole(ROWS, 2 * feat), cols, cols, down, third(0), third(1), third(2), whole(late, 2 * feat)],
        out_specs=[whole(ROWS, feat), whole(ROWS, feat), cols, cols, down],
        scratch_shapes=[buf(feat, late)],
    )(both, gg, gu, gd, hid, hid, hid, tc)


def solution(mesh):
    placed = (P("mp", "dp"), P("mp", "dp"), P("dp", "mp"), P("dp", "mp"), P("mp", "dp"))
    return jax.shard_map(
        per_device, mesh=mesh, in_specs=placed, out_specs=placed, check_vma=False
    )
```

```python
import jax
import jax.numpy as jnp
from jax import lax
from jax.experimental import pallas as pl
from jax.experimental.pallas import tpu as pltpu
from jax.sharding import PartitionSpec as P

MESH = pl.DeviceIdType.MESH
F32 = jnp.float32
BF16 = jnp.bfloat16
ROWS = 128
TILE = 256

CHUNKS = ((1, 1), (3, 1), (2, 1), (1, 0), (0, 1), (3, 0), (2, 0), (0, 0))
NUMBER = {c: i for i, c in enumerate(CHUNKS)}
EARLY = 4
PIECES = (6, 7)
FIRST = NUMBER[0, 0]
ORDER = (
    (0,), (5, 7), (6, 7), (7, 7), (8, 7), (2, 0), (5, 3), (1,), (9, 7), (3, 0), (10, 7), (6, 3), (5, 4),
    (6, 4), (11, 7), (7, 3), (5, 6), (7, 4), (8, 3), (6, 6), (8, 4), (7, 6), (10, 3), (9, 3), (3, 1), (5, 2),
    (9, 4), (2, 1), (8, 6), (5, 0), (10, 4), (6, 0), (11, 3), (6, 2), (4, 0), (7, 2), (8, 2), (5, 5), (7, 0),
    (11, 6), (8, 0), (9, 6), (4, 1), (5, 1), (12, 3), (13, 3), (9, 2), (10, 2), (11, 2), (13, 7), (9, 0),
    (6, 1), (7, 1), (6, 5), (10, 0), (8, 1), (13, 2), (12, 4), (11, 0), (12, 2), (13, 6), (7, 5), (8, 5),
    (9, 1), (11, 4), (10, 1), (11, 1), (13, 0), (10, 6), (12, 0), (14, 2), (9, 5), (10, 5), (12, 1), (13, 1),
    (14, 3), (14, 0), (11, 5), (14, 1), (15, 2), (16, 3), (16, 2), (13, 4), (13, 5), (15, 0), (12, 5), (15, 1),
    (16, 1), (12, 6), (16, 0), (15, 3), (18, 3), (17, 2), (14, 5), (18, 1), (17, 1), (17, 0), (18, 0), (14, 4),
    (18, 2), (15, 5), (16, 5), (14, 6), (19, 1), (17, 3), (19, 0), (20, 0), (20, 1), (12, 7), (15, 4), (19, 2),
    (20, 2), (21, 1), (16, 4), (17, 5), (22, 3, 1), (18, 5), (15, 6), (16, 6), (21, 0), (14, 7), (21, 2),
    (19, 3), (22, 1, 1), (18, 4), (20, 3), (22, 2, 1), (17, 4), (19, 5), (20, 5), (23, 2, 1), (18, 6), (17, 6),
    (23, 1, 1), (21, 3), (26, 0), (16, 7), (15, 7), (19, 4), (21, 5), (22, 3, 0), (20, 4), (19, 6), (20, 6),
    (22, 1, 0), (26, 1), (18, 7), (21, 4), (24,), (21, 6), (22, 2, 0), (17, 7), (26, 2), (26, 3), (23, 1, 0),
    (23, 2, 0), (26, 4), (19, 7), (20, 7), (26, 5), (21, 7), (25,),
)


def dot(a, b, ca, cb):
    return lax.dot_general(a, b, (((ca,), (cb,)), ((), ())), preferred_element_type=F32)


def at_rows(start, size, step):
    return pl.ds(pl.multiple_of(start, step), size)


def exchange(
    tok_hbm, cot_hbm, wg_hbm, wu_hbm, wd_hbm,
    both, gg, gu, gd, hid, tc,
    wg, wu, wd, part, cin, midl, midr, xl, xr, fo, zs, zr, zd, dmid, dxl, dxr, acc,
    o, yml, ymr, yl, yr, yzs, yzr,
    send_sem, recv_sem, copy_sem,
):
    feat, ff = wg.shape
    half = ff // 2
    gu_cols, dh_cols = slice(0, 2 * half), slice(2 * half, 3 * half)
    dp, mp = lax.axis_index("dp"), lax.axis_index("mp")
    zl, x, k = dp // 8, (dp // 2) % 4, dp % 2
    zh, y = mp // 4, mp % 4
    xp, xm, x2 = (x + 1) % 4, (x + 3) % 4, (x + 2) % 4
    core = (zl * 8 + x * 2 + 1 - k, mp)
    right = (zl * 8 + xp * 2 + k, mp)
    left = (zl * 8 + xm * 2 + k, mp)
    zpeer = ((1 - zl) * 8 + x * 2 + k, mp)
    up_y = (dp, zh * 4 + (y + 1) % 4)
    dn_y = (dp, zh * 4 + (y + 3) % 4)
    zhpeer = (dp, (1 - zh) * 4 + y)

    local = []

    def fetch(src, dst):
        copy = pltpu.make_async_copy(src, dst, copy_sem.at[len(local)])
        copy.start()
        local.append(copy)
        return copy

    own = slice(NUMBER[0, 0] * ROWS, (NUMBER[0, 0] + 1) * ROWS)
    inputs = [fetch(tok_hbm, tc.at[own, :feat]), fetch(cot_hbm, tc.at[own, feat:])]
    weights = [fetch(wg_hbm, wg), fetch(wu_hbm, wu), fetch(wd_hbm, wd)]
    barrier = pltpu.get_barrier_semaphore()
    peers = (core, right, left, zpeer, up_y, dn_y, zhpeer)
    for p in peers:
        pl.semaphore_signal(barrier, inc=1, device_id=p, device_id_type=MESH)

    sent = []
    names = {}

    def sem(name):
        return names.setdefault(name, len(names))

    def send(name, src, dst, device, index=None):
        at = sem(name) if index is None else index
        copy = pltpu.make_async_remote_copy(
            src_ref=src, dst_ref=dst, send_sem=send_sem.at[len(sent)], recv_sem=recv_sem.at[at],
            device_id=device, device_id_type=MESH,
        )
        copy.start()
        sent.append(copy)

    def recv(name, ref, index=None):
        at = sem(name) if index is None else index
        pltpu.make_async_remote_copy(
            src_ref=ref, dst_ref=ref, send_sem=send_sem.at[0], recv_sem=recv_sem.at[at],
            device_id=core, device_id_type=MESH,
        ).wait_recv()

    def chunk(c):
        return slice(c * ROWS, (c + 1) * ROWS)

    def tokens(slot, rel, piece=slice(0, ROWS)):
        base = NUMBER[slot, rel] * ROWS
        return tc.at[base + piece.start : base + piece.stop]

    lo, hi = slice(0, ROWS // 2), slice(ROWS // 2, ROWS)

    def start():
        for copy in inputs:
            copy.wait()
        pl.semaphore_wait(barrier, len(peers))
        send("t01", tokens(0, 0), tokens(0, 1), zhpeer)
        send(("t1", 0), tokens(0, 0), tokens(1, 0), dn_y)
        send(("t2", 0), tokens(0, 0), tokens(2, 0), up_y)

    def gather_a():
        recv("t01", tokens(0, 1))
        send(("t1", 1), tokens(0, 1), tokens(1, 1), dn_y)
        send(("t2", 1), tokens(0, 1), tokens(2, 1), up_y)

    def gather_b(rel):
        recv(("t1", rel), tokens(1, rel))
        send(("t3", rel, "a"), tokens(1, rel, lo), tokens(3, rel, lo), dn_y)

    def gather_b2(rel):
        recv(("t2", rel), tokens(2, rel))
        send(("t3", rel, "b"), tokens(2, rel, hi), tokens(3, rel, hi), up_y)

    def gather_c(rel):
        recv(("t3", rel, "a"), tokens(3, rel, lo))
        recv(("t3", rel, "b"), tokens(3, rel, hi))

    def products(c, q):
        here = chunk(c)
        c0 = at_rows(q * half, half, 128)

        def arrived():
            if weights:
                weights.pop(0).wait()

        arrived()
        part[q, here, :half] = dot(tc[here, :feat], wg[:, c0], 1, 0).astype(BF16)
        arrived()
        part[q, here, half : 2 * half] = dot(tc[here, :feat], wu[:, c0], 1, 0).astype(BF16)
        arrived()
        part[q, here, 2 * half :] = dot(tc[here, feat:], wd[c0, :], 1, 1).astype(BF16)

    pieces = ((x2, 0), (x2, 1), (xp, 1), (xm, 0), (xp, 0), (xm, 1), (x, 0), (x, 1))

    def first(c):
        products(c, 1 - k)
        if c == FIRST:
            for i, (xx, zz) in enumerate(pieces):
                r = at_rows(zz * 64 + xx * 16, 16, 16)
                send(("c", c, i), part.at[1 - k, piece(c, xx, zz)], cin.at[c, r], core)
        else:
            send(("c", c), part.at[1 - k, chunk(c)], cin.at[c], core)

    def piece_in(c, i):
        if c == FIRST:
            xx, zz = pieces[i]
            recv(("c", c, i), cin.at[c, at_rows(zz * 64 + xx * 16, 16, 16)])

    def second(c):
        products(c, k)

    def piece(c, xx, zz):
        return at_rows(c * ROWS + zz * 64 + xx * 16, 16, 16)

    thirds = [slice(j * half, (j + 1) * half) for j in range(3)]

    def add_to(r, cols, other):
        part[k, r, cols] = (part[k, r, cols].astype(F32) + other.astype(F32)).astype(BF16)

    def core_sum(c, xx, zz):
        for cols in thirds[:2]:
            add_to(piece(c, xx, zz), cols, cin[c, at_rows(zz * 64 + xx * 16, 16, 16), cols])

    def core_sum_dh(c, zz):
        @pl.loop(0, 4)
        def _(i):
            add_to(piece(c, i, zz), dh_cols, cin[c, at_rows(zz * 64 + i * 16, 16, 16), dh_cols])

    def gu_part(r):
        return part.at[k, r, gu_cols]

    def dh_part(r):
        return part.at[k, r, dh_cols]

    def sum1(c):
        if c != FIRST:
            recv(("c", c), cin.at[c])
        piece_in(c, 0)
        core_sum(c, x2, 0)
        send(("ml", c), gu_part(piece(c, x2, 0)), midl.at[c], right)
        piece_in(c, 1)
        core_sum(c, x2, 1)
        send(("mr", c), gu_part(piece(c, x2, 1)), midr.at[c], left)
        piece_in(c, 2)
        core_sum(c, xp, 1)
        send(("xl", c, 1), gu_part(piece(c, xp, 1)), xl.at[c, 1], right)
        piece_in(c, 3)
        core_sum(c, xm, 0)
        send(("xr", c, 0), gu_part(piece(c, xm, 0)), xr.at[c, 0], left)

    def sum1b(c):
        for i in range(4, 8):
            piece_in(c, i)
        core_sum_dh(c, 1 - zl)
        send(("zd", c), dh_part(at_rows(c * ROWS + (1 - zl) * 64, 64, 64)), zd.at[c], zpeer)
        core_sum(c, xp, 0)
        core_sum(c, xm, 1)
        core_sum(c, x, 0)
        core_sum(c, x, 1)
        core_sum_dh(c, zl)

    def sum2a(c):
        recv(("ml", c), midl.at[c])
        for cols in thirds[:2]:
            add_to(piece(c, xp, 0), cols, midl[c, :, cols])
        send(("xl", c, 0), gu_part(piece(c, xp, 0)), xl.at[c, 0], right)

    def sum2b(c):
        recv(("mr", c), midr.at[c])
        for cols in thirds[:2]:
            add_to(piece(c, xm, 1), cols, midr[c, :, cols])
        send(("xr", c, 1), gu_part(piece(c, xm, 1)), xr.at[c, 1], left)

    def sum2c(c):
        recv(("zd", c), zd.at[c])

        def add_dh(xx):
            add_to(piece(c, xx, zl), dh_cols, zd[c, at_rows(xx * 16, 16, 16), :])

        add_dh(x2)
        far = dh_part(piece(c, x2, zl))
        if c % 2:
            send(("dm", c), far, dmid.at[c], left)
            add_dh(xp)
            send(("dl", c), dh_part(piece(c, xp, zl)), dxl.at[c], right)
            add_dh(xm)
        else:
            send(("dm", c), far, dmid.at[c], right)
            add_dh(xm)
            send(("dr", c), dh_part(piece(c, xm, zl)), dxr.at[c], left)
            add_dh(xp)
        add_dh(x)

    def sum3a(c):
        recv(("xl", c, 1), xl.at[c, 1])
        recv(("xr", c, 0), xr.at[c, 0])
        recv(("xl", c, 0), xl.at[c, 0])
        recv(("xr", c, 1), xr.at[c, 1])
        for cols in thirds[:2]:
            zs[c, :, cols] = (
                part[k, piece(c, x, 1 - zl), cols].astype(F32)
                + xl[c, 1 - zl, :, cols].astype(F32)
                + xr[c, 1 - zl, :, cols].astype(F32)
            ).astype(BF16)
        send(("zz", c), zs.at[c], zr.at[c], zpeer)
        for cols in thirds[:2]:
            fo[c, :, cols] = (
                part[k, piece(c, x, zl), cols].astype(F32)
                + xl[c, zl, :, cols].astype(F32)
                + xr[c, zl, :, cols].astype(F32)
            )

    def sum3b(c):
        recv(("dm", c), dmid.at[c])
        if c % 2:
            add_to(piece(c, xm, zl), dh_cols, dmid[c])
            send(("dr", c), dh_part(piece(c, xm, zl)), dxr.at[c], left)
        else:
            add_to(piece(c, xp, zl), dh_cols, dmid[c])
            send(("dl", c), dh_part(piece(c, xp, zl)), dxl.at[c], right)

    def middle(c):
        recv(("zz", c), zr.at[c])
        recv(("dl", c), dxl.at[c])
        recv(("dr", c), dxr.at[c])
        r = piece(c, x, zl)

        @pl.loop(0, half // 128)
        def _(n):
            c0, c1, c2 = (at_rows(j * half + n * 128, 128, 128) for j in range(3))
            gate = fo[c, :, c0] + zr[c, :, c0].astype(F32)
            up = fo[c, :, c1] + zr[c, :, c1].astype(F32)
            dh = part[k, r, c2].astype(F32) + dxl[c, :, c0].astype(F32) + dxr[c, :, c0].astype(F32)
            sig = 1.0 / (1.0 + jnp.exp(-gate))
            act = gate * sig
            hid[k, r, c0] = (act * up).astype(BF16)
            hid[k, r, c1] = (dh * up * sig * (1.0 + gate * (1.0 - sig))).astype(BF16)
            hid[k, r, c2] = (dh * act).astype(BF16)

        full = hid.at[k, r]
        send("", full, full, right, sem(("gl", c)) + zl)
        sem(("gl", c, "b"))
        send("", full, full, left, sem(("gr", c)) + zl)
        sem(("gr", c, "b"))
        send(("gz", c), full, full, zpeer)

    def pass_on(name, r, cols, device, index=None):
        ref = hid.at[k, r, cols]
        send(name, ref, ref, device, index)

    def spread1(c):
        gl, gr = sem(("gl", c)), sem(("gr", c))
        other = piece(c, x, 1 - zl)
        recv(("gz", c), hid.at[k, other])
        pass_on("", other, gu_cols, right, gl + 1 - zl)
        pass_on("", other, gu_cols, left, gr + 1 - zl)

    def spread2a(c):
        gl, gr = sem(("gl", c)), sem(("gr", c))
        recv("", hid.at[k, piece(c, xm, zl)], gl + zl)
        recv("", hid.at[k, piece(c, xp, zl)], gr + zl)
        if c % 2:
            pass_on(("fd", c), piece(c, xp, zl), dh_cols, left)
        else:
            pass_on(("fd", c), piece(c, xm, zl), dh_cols, right)
        pass_on(("du", c, "m"), piece(c, xm, zl), dh_cols, zpeer)
        pass_on(("du", c, "p"), piece(c, xp, zl), dh_cols, zpeer)

    def spread2b(c):
        gl, gr = sem(("gl", c)), sem(("gr", c))
        recv("", hid.at[k, piece(c, xm, 1 - zl), gu_cols], gl + 1 - zl)
        recv("", hid.at[k, piece(c, xp, 1 - zl), gu_cols], gr + 1 - zl)
        pass_on(("fl", c), piece(c, xm, 0), gu_cols, right)
        pass_on(("fr", c), piece(c, xp, 1), gu_cols, left)
        if c in PIECES:
            to_core(c, 0, ((x, 0), (x, 1), (xm, zl), (xp, zl)))

    def to_core(c, base, places):
        for i, (xx, zz) in enumerate(places):
            ref = hid.at[k, piece(c, xx, zz)]
            send(("gc", c, base + i), ref, ref, core)

    def from_core(c, base, places):
        for i, (xx, zz) in enumerate(places):
            recv(("gc", c, base + i), hid.at[1 - k, piece(c, xx, zz)])

    def spread3(c):
        recv(("fd", c), hid.at[k, piece(c, x2, zl), dh_cols])
        pass_on(("du", c, "f"), piece(c, x2, zl), dh_cols, zpeer)

    def spread4(c):
        recv(("fl", c), hid.at[k, piece(c, x2, 0), gu_cols])
        recv(("fr", c), hid.at[k, piece(c, x2, 1), gu_cols])
        recv(("du", c, "m"), hid.at[k, piece(c, xm, 1 - zl), dh_cols])
        recv(("du", c, "p"), hid.at[k, piece(c, xp, 1 - zl), dh_cols])
        recv(("du", c, "f"), hid.at[k, piece(c, x2, 1 - zl), dh_cols])
        if c in PIECES:
            to_core(c, 4, ((xm, 1 - zl), (xp, 1 - zl), (x2, 0), (x2, 1)))
        else:
            send(("gc", c), hid.at[k, chunk(c)], hid.at[k, chunk(c)], core)

    def last_terms(c, q):
        here = chunk(c)
        c0 = at_rows(q * half, half, 128)
        return dot(hid[q, here, thirds[0]], wd[c0, :], 1, 0), (
            dot(hid[q, here, thirds[1]], wg[:, c0], 1, 1) + dot(hid[q, here, thirds[2]], wu[:, c0], 1, 1)
        )

    def last1(c):
        a, b = last_terms(c, k)
        acc[chunk(c), :feat] = a
        acc[chunk(c), feat:] = b

    def last2(c):
        if c in PIECES:
            from_core(c, 0, ((x, 0), (x, 1), (xm, zl), (xp, zl)))
            from_core(c, 4, ((xm, 1 - zl), (xp, 1 - zl), (x2, 0), (x2, 1)))
        else:
            recv(("gc", c), hid.at[1 - k, chunk(c)])
        here = chunk(c)
        a, b = last_terms(c, 1 - k)
        o[here, :feat] = (acc[here, :feat] + a).astype(BF16)
        o[here, feat:] = (acc[here, feat:] + b).astype(BF16)

    def out_rows(slot, rel, piece):
        base = NUMBER[slot, rel] * ROWS
        return slice(base + piece.start, base + piece.stop)

    def send_out(name, slot, rel, piece, dst, device):
        send(name, o.at[out_rows(slot, rel, piece)], dst, device)

    def add_out(slot, rel, piece, other):
        r = out_rows(slot, rel, piece)
        o[r] = (o[r].astype(F32) + other.astype(F32)).astype(BF16)

    def out(slot, rel):
        if slot == 3:
            send_out(("ym", rel, "l"), 3, rel, lo, yml.at[rel], up_y)
            send_out(("ym", rel, "r"), 3, rel, hi, ymr.at[rel], dn_y)
        if slot == 1:
            send_out(("yl", rel, "h"), 1, rel, hi, yl.at[rel, hi], up_y)
        if slot == 2:
            send_out(("yr", rel, "l"), 2, rel, lo, yr.at[rel, lo], dn_y)

    def relay(slot, rel):
        if slot == 1:
            recv(("ym", rel, "l"), yml.at[rel])
            add_out(1, rel, lo, yml[rel])
            send_out(("yl", rel, "l"), 1, rel, lo, yl.at[rel, lo], up_y)
        else:
            recv(("ym", rel, "r"), ymr.at[rel])
            add_out(2, rel, hi, ymr[rel])
            send_out(("yr", rel, "h"), 2, rel, hi, yr.at[rel, hi], dn_y)

    def gather_out(rel):
        recv(("yl", rel, "h"), yl.at[rel, hi])
        recv(("yr", rel, "l"), yr.at[rel, lo])
        recv(("yl", rel, "l"), yl.at[rel, lo])
        recv(("yr", rel, "h"), yr.at[rel, hi])
        r = chunk(NUMBER[0, rel])
        return o[r].astype(F32) + yl[rel].astype(F32) + yr[rel].astype(F32)

    def finish1():
        yzs[...] = gather_out(1).astype(BF16)
        send("yz", yzs, yzr, zhpeer)

    def finish0():
        total = gather_out(0)
        recv("yz", yzr)
        both[...] = (total + yzr[...].astype(F32)).astype(BF16)

    rows_early = slice(0, EARLY * ROWS)

    def grad(i):
        if i < 4:
            q, m = i // 2, i % 2
            c = slice(q * half, (q + 1) * half)
            f = slice(m * feat // 2, (m + 1) * feat // 2)
            a = tc[rows_early, f]
            gg[f, c] = dot(a, hid[q, rows_early, thirds[1]], 0, 0).astype(BF16)
            gu[f, c] = dot(a, hid[q, rows_early, thirds[2]], 0, 0).astype(BF16)
        else:
            q = i - 4

            @pl.loop(0, half // 128)
            def _(n):
                h = hid[q, rows_early, at_rows(n * 128, 128, 128)]
                gd[at_rows(q * half + n * 128, 128, 128), :] = dot(
                    h, tc[rows_early, feat:], 0, 0
                ).astype(BF16)

    steps = (
        start, gather_a, gather_b, gather_b2, gather_c, first, second, sum1, sum1b, sum2a, sum2b, sum2c, sum3a, sum3b, middle, spread1, spread2a, spread2b, spread3, spread4, last1, last2, out, relay, finish1, finish0, grad,
    )
    for number, *arguments in ORDER:
        steps[number](*arguments)
    for copy in sent:
        copy.wait_send()


def finish(both, gg_in, gu_in, gd_in, hid, tc, out, gin, gg, gu, gd, bv, ga, ua, da, turned, out_sem):
    feat, ff = gg_in.shape
    half = ff // 2
    rows = slice(EARLY * ROWS, tc.shape[0])
    leaving = []

    def leave(src, dst):
        copy = pltpu.make_async_copy(src, dst, out_sem.at[len(leaving)])
        copy.start()
        leaving.append(copy)

    bv[...] = both[...]
    leave(bv.at[:, :feat], out)
    leave(bv.at[:, feat:], gin)
    turned[...] = tc[rows, :feat].T
    for third, before, total, dst in ((1, gg_in, ga, gg), (2, gu_in, ua, gu)):
        for f in (slice(n * TILE, (n + 1) * TILE) for n in range(feat // TILE)):
            for q in range(2):
                c = slice(q * half, (q + 1) * half)
                more = dot(turned[f], hid[q, rows, third * half : (third + 1) * half], 1, 0)
                total[f, c] = (before[f, c].astype(F32) + more).astype(BF16)
            leave(total.at[f], dst.at[f])
    step = 128
    for q in range(2):
        for n in range(half // step):
            u = slice(q * half + n * step, q * half + (n + 1) * step)
            more = dot(hid[q, rows, n * step : (n + 1) * step], tc[rows, feat:], 0, 0)
            da[u] = (gd_in[u].astype(F32) + more).astype(BF16)
            leave(da.at[u], gd.at[u])
    for copy in leaving:
        copy.wait()


def per_device(tokens, cotangent, gate_weight, up_weight, down_weight):
    feat, ff = gate_weight.shape
    half = ff // 2
    count = 8 * ROWS
    vmem = pl.BlockSpec(memory_space=pltpu.VMEM)
    hbm = pl.BlockSpec(memory_space=pl.ANY)
    shape = lambda *s: jax.ShapeDtypeStruct(s, BF16)
    buf = lambda *s: pltpu.VMEM(s, BF16)
    kept = pl.pallas_call(
        exchange,
        out_shape=(
            buf(ROWS, 2 * feat), buf(feat, ff), buf(feat, ff), buf(ff, feat),
            buf(2, count, 3 * half), buf(count, 2 * feat),
        ),
        in_specs=[hbm] * 5,
        out_specs=[vmem] * 6,
        scratch_shapes=[
            buf(feat, ff), buf(feat, ff), buf(ff, feat),
            buf(2, count, 3 * half), buf(8, ROWS, 3 * half),
            buf(8, 16, 2 * half), buf(8, 16, 2 * half),
            buf(8, 2, 16, 2 * half), buf(8, 2, 16, 2 * half),
            pltpu.VMEM((8, 16, 2 * half), F32), buf(8, 16, 2 * half), buf(8, 16, 2 * half),
            buf(8, 64, half), buf(8, 16, half), buf(8, 16, half), buf(8, 16, half),
            pltpu.VMEM((count, 2 * feat), F32), buf(count, 2 * feat),
            buf(2, 64, 2 * feat), buf(2, 64, 2 * feat),
            buf(2, ROWS, 2 * feat), buf(2, ROWS, 2 * feat),
            buf(ROWS, 2 * feat), buf(ROWS, 2 * feat),
            pltpu.SemaphoreType.DMA((304,)), pltpu.SemaphoreType.DMA((304,)), pltpu.SemaphoreType.DMA((8,)),
        ],
        compiler_params=pltpu.CompilerParams(
            collective_id=0, has_side_effects=True, vmem_limit_bytes=40 * 2**20
        ),
    )(tokens, cotangent, gate_weight, up_weight, down_weight)
    return pl.pallas_call(
        finish,
        out_shape=(shape(ROWS, feat), shape(ROWS, feat), shape(feat, ff), shape(feat, ff), shape(ff, feat)),
        in_specs=[vmem] * 6,
        out_specs=[hbm] * 5,
        scratch_shapes=[
            buf(ROWS, 2 * feat), buf(feat, ff), buf(feat, ff), buf(ff, feat),
            buf(feat, count - EARLY * ROWS),
            pltpu.SemaphoreType.DMA((2 * feat // TILE + ff // 128 + 2,)),
        ],
        compiler_params=pltpu.CompilerParams(vmem_limit_bytes=12 * 2**20),
    )(*kept)


def solution(mesh):
    placed = (P("mp", "dp"), P("mp", "dp"), P("dp", "mp"), P("dp", "mp"), P("mp", "dp"))
    return jax.shard_map(
        per_device, mesh=mesh, in_specs=placed, out_specs=placed, check_vma=False
    )
```

```python
import jax
import jax.numpy as jnp
from jax import lax
from jax.experimental import pallas as pl
from jax.experimental.pallas import tpu as pltpu
from jax.sharding import PartitionSpec as P

MESH = pl.DeviceIdType.MESH
F32 = jnp.float32
BF16 = jnp.bfloat16
ROWS = 128
TILE = 256

CHUNKS = ((1, 1), (3, 1), (0, 1), (3, 0), (1, 0), (2, 1), (2, 0), (0, 0))
NUMBER = {c: i for i, c in enumerate(CHUNKS)}
EARLY = 4
PIECES = (6, 7)
FIRST = NUMBER[0, 0]
ORDER = (
    (0,), (5, 7), (6, 7), (7, 7), (8, 7), (2, 0), (5, 4), (3, 0), (10, 7), (1,), (5, 2), (9, 7), (6, 2),
    (5, 6), (6, 4), (11, 7), (7, 4), (8, 4), (7, 2), (8, 2), (4, 0), (5, 3), (6, 6), (6, 3), (7, 6), (2, 1),
    (7, 3), (8, 3), (12, 7), (5, 0), (3, 1), (8, 6), (6, 0), (10, 4), (11, 4), (11, 2), (9, 4), (5, 5), (9, 3),
    (10, 2), (7, 0), (6, 5), (8, 0), (10, 3), (10, 6), (11, 3), (4, 1), (5, 1), (6, 1), (13, 2), (12, 4),
    (9, 2), (10, 0), (9, 0), (11, 0), (7, 1), (8, 1), (13, 3), (12, 3), (7, 5), (8, 5), (9, 1), (10, 1),
    (9, 6), (12, 2), (9, 5), (11, 1), (14, 3), (12, 0), (10, 5), (12, 1), (11, 5), (13, 1), (14, 2), (13, 0),
    (12, 6), (15, 3), (13, 5), (11, 6), (12, 5), (14, 1), (13, 4), (14, 0), (14, 5), (16, 1), (15, 1), (15, 0),
    (16, 3), (16, 0), (13, 6), (15, 5), (16, 5), (16, 2), (17, 1), (18, 1), (14, 4), (18, 0), (17, 5), (18, 3),
    (18, 5), (17, 0), (14, 6), (15, 2), (19, 1), (18, 2), (17, 3), (16, 4), (20, 1), (15, 4), (19, 5), (20, 5),
    (21, 1), (22, 3, 1), (15, 6), (19, 0), (13, 7), (20, 0), (17, 2), (21, 5), (16, 6), (21, 0), (19, 3),
    (22, 1, 1), (18, 4), (23, 1, 1, 0), (17, 4), (20, 3), (23, 1, 1, 1), (23, 2, 1, 0), (22, 2, 1), (17, 6),
    (14, 7), (19, 2), (18, 6), (23, 2, 1, 1), (20, 2), (19, 4), (20, 4), (21, 3), (22, 3, 0), (15, 7), (21, 2),
    (19, 6), (20, 6), (16, 7), (24, 0), (26, 0), (21, 4), (21, 6), (22, 2, 0), (22, 1, 0), (17, 7), (26, 1),
    (18, 7), (24, 1), (23, 2, 0, 0), (23, 1, 0, 0), (23, 1, 0, 1), (26, 2), (26, 3), (23, 2, 0, 1), (26, 4),
    (19, 7), (20, 7), (26, 5), (21, 7), (25, 0), (25, 1),
)


def dot(a, b, ca, cb):
    return lax.dot_general(a, b, (((ca,), (cb,)), ((), ())), preferred_element_type=F32)


def at_rows(start, size, step):
    return pl.ds(pl.multiple_of(start, step), size)


def exchange(
    tok_hbm, cot_hbm, wg_hbm, wu_hbm, wd_hbm,
    both, gg, gu, gd, hid, tc,
    wg, wu, wd, part, cin, midl, midr, xl, xr, fo, zs, zr, zd, dmid, dxl, dxr, acc,
    o, yml, ymr, yl, yr, yzs, yzr,
    send_sem, recv_sem, copy_sem,
):
    feat, ff = wg.shape
    half = ff // 2
    gu_cols, dh_cols = slice(0, 2 * half), slice(2 * half, 3 * half)
    dp, mp = lax.axis_index("dp"), lax.axis_index("mp")
    zl, x, k = dp // 8, (dp // 2) % 4, dp % 2
    zh, y = mp // 4, mp % 4
    xp, xm, x2 = (x + 1) % 4, (x + 3) % 4, (x + 2) % 4
    core = (zl * 8 + x * 2 + 1 - k, mp)
    right = (zl * 8 + xp * 2 + k, mp)
    left = (zl * 8 + xm * 2 + k, mp)
    zpeer = ((1 - zl) * 8 + x * 2 + k, mp)
    up_y = (dp, zh * 4 + (y + 1) % 4)
    dn_y = (dp, zh * 4 + (y + 3) % 4)
    zhpeer = (dp, (1 - zh) * 4 + y)

    local = []

    def fetch(src, dst):
        copy = pltpu.make_async_copy(src, dst, copy_sem.at[len(local)])
        copy.start()
        local.append(copy)
        return copy

    own = slice(NUMBER[0, 0] * ROWS, (NUMBER[0, 0] + 1) * ROWS)
    inputs = [fetch(tok_hbm, tc.at[own, :feat]), fetch(cot_hbm, tc.at[own, feat:])]
    weights = [fetch(wg_hbm, wg), fetch(wu_hbm, wu), fetch(wd_hbm, wd)]
    barrier = pltpu.get_barrier_semaphore()
    peers = (core, right, left, zpeer, up_y, dn_y, zhpeer)
    for p in peers:
        pl.semaphore_signal(barrier, inc=1, device_id=p, device_id_type=MESH)

    sent = []
    names = {}

    def sem(name):
        return names.setdefault(name, len(names))

    def send(name, src, dst, device, index=None):
        at = sem(name) if index is None else index
        copy = pltpu.make_async_remote_copy(
            src_ref=src, dst_ref=dst, send_sem=send_sem.at[len(sent)], recv_sem=recv_sem.at[at],
            device_id=device, device_id_type=MESH,
        )
        copy.start()
        sent.append(copy)

    def recv(name, ref, index=None):
        at = sem(name) if index is None else index
        pltpu.make_async_remote_copy(
            src_ref=ref, dst_ref=ref, send_sem=send_sem.at[0], recv_sem=recv_sem.at[at],
            device_id=core, device_id_type=MESH,
        ).wait_recv()

    def chunk(c):
        return slice(c * ROWS, (c + 1) * ROWS)

    def tokens(slot, rel, piece=slice(0, ROWS)):
        base = NUMBER[slot, rel] * ROWS
        return tc.at[base + piece.start : base + piece.stop]

    lo, hi = slice(0, ROWS // 2), slice(ROWS // 2, ROWS)

    def start():
        for copy in inputs:
            copy.wait()
        pl.semaphore_wait(barrier, len(peers))
        send("t01", tokens(0, 0), tokens(0, 1), zhpeer)
        send(("t1", 0), tokens(0, 0), tokens(1, 0), dn_y)
        send(("t2", 0), tokens(0, 0), tokens(2, 0), up_y)

    def gather_a():
        recv("t01", tokens(0, 1))
        send(("t1", 1), tokens(0, 1), tokens(1, 1), dn_y)
        send(("t2", 1), tokens(0, 1), tokens(2, 1), up_y)

    def gather_b(rel):
        recv(("t1", rel), tokens(1, rel))
        send(("t3", rel, "a"), tokens(1, rel, lo), tokens(3, rel, lo), dn_y)

    def gather_b2(rel):
        recv(("t2", rel), tokens(2, rel))
        send(("t3", rel, "b"), tokens(2, rel, hi), tokens(3, rel, hi), up_y)

    def gather_c(rel):
        recv(("t3", rel, "a"), tokens(3, rel, lo))
        recv(("t3", rel, "b"), tokens(3, rel, hi))

    def products(c, q):
        here = chunk(c)
        c0 = at_rows(q * half, half, 128)

        def arrived():
            if weights:
                weights.pop(0).wait()

        arrived()
        part[q, here, :half] = dot(tc[here, :feat], wg[:, c0], 1, 0).astype(BF16)
        arrived()
        part[q, here, half : 2 * half] = dot(tc[here, :feat], wu[:, c0], 1, 0).astype(BF16)
        arrived()
        part[q, here, 2 * half :] = dot(tc[here, feat:], wd[c0, :], 1, 1).astype(BF16)

    pieces = ((x2, 0), (x2, 1), (xp, 1), (xm, 0), (xp, 0), (xm, 1), (x, 0), (x, 1))

    def first(c):
        products(c, 1 - k)
        if c == FIRST:
            for i, (xx, zz) in enumerate(pieces):
                r = at_rows(zz * 64 + xx * 16, 16, 16)
                send(("c", c, i), part.at[1 - k, piece(c, xx, zz)], cin.at[c, r], core)
        else:
            send(("c", c), part.at[1 - k, chunk(c)], cin.at[c], core)

    def piece_in(c, i):
        if c == FIRST:
            xx, zz = pieces[i]
            recv(("c", c, i), cin.at[c, at_rows(zz * 64 + xx * 16, 16, 16)])

    def second(c):
        products(c, k)

    def piece(c, xx, zz):
        return at_rows(c * ROWS + zz * 64 + xx * 16, 16, 16)

    thirds = [slice(j * half, (j + 1) * half) for j in range(3)]

    def add_to(r, cols, other):
        part[k, r, cols] = (part[k, r, cols].astype(F32) + other.astype(F32)).astype(BF16)

    def core_sum(c, xx, zz):
        for cols in thirds[:2]:
            add_to(piece(c, xx, zz), cols, cin[c, at_rows(zz * 64 + xx * 16, 16, 16), cols])

    def core_sum_dh(c, zz):
        @pl.loop(0, 4)
        def _(i):
            add_to(piece(c, i, zz), dh_cols, cin[c, at_rows(zz * 64 + i * 16, 16, 16), dh_cols])

    def gu_part(r):
        return part.at[k, r, gu_cols]

    def dh_part(r):
        return part.at[k, r, dh_cols]

    def sum1(c):
        if c != FIRST:
            recv(("c", c), cin.at[c])
        piece_in(c, 0)
        core_sum(c, x2, 0)
        send(("ml", c), gu_part(piece(c, x2, 0)), midl.at[c], right)
        piece_in(c, 1)
        core_sum(c, x2, 1)
        send(("mr", c), gu_part(piece(c, x2, 1)), midr.at[c], left)
        piece_in(c, 2)
        core_sum(c, xp, 1)
        send(("xl", c, 1), gu_part(piece(c, xp, 1)), xl.at[c, 1], right)
        piece_in(c, 3)
        core_sum(c, xm, 0)
        send(("xr", c, 0), gu_part(piece(c, xm, 0)), xr.at[c, 0], left)

    def sum1b(c):
        for i in range(4, 8):
            piece_in(c, i)
        core_sum_dh(c, 1 - zl)
        send(("zd", c), dh_part(at_rows(c * ROWS + (1 - zl) * 64, 64, 64)), zd.at[c], zpeer)
        core_sum(c, xp, 0)
        core_sum(c, xm, 1)
        core_sum(c, x, 0)
        core_sum(c, x, 1)
        core_sum_dh(c, zl)

    def sum2a(c):
        recv(("ml", c), midl.at[c])
        for cols in thirds[:2]:
            add_to(piece(c, xp, 0), cols, midl[c, :, cols])
        send(("xl", c, 0), gu_part(piece(c, xp, 0)), xl.at[c, 0], right)

    def sum2b(c):
        recv(("mr", c), midr.at[c])
        for cols in thirds[:2]:
            add_to(piece(c, xm, 1), cols, midr[c, :, cols])
        send(("xr", c, 1), gu_part(piece(c, xm, 1)), xr.at[c, 1], left)

    def sum2c(c):
        recv(("zd", c), zd.at[c])

        def add_dh(xx):
            add_to(piece(c, xx, zl), dh_cols, zd[c, at_rows(xx * 16, 16, 16), :])

        add_dh(x2)
        far = dh_part(piece(c, x2, zl))
        if c % 2:
            send(("dm", c), far, dmid.at[c], left)
            add_dh(xp)
            send(("dl", c), dh_part(piece(c, xp, zl)), dxl.at[c], right)
            add_dh(xm)
        else:
            send(("dm", c), far, dmid.at[c], right)
            add_dh(xm)
            send(("dr", c), dh_part(piece(c, xm, zl)), dxr.at[c], left)
            add_dh(xp)
        add_dh(x)

    def sum3a(c):
        recv(("xl", c, 1), xl.at[c, 1])
        recv(("xr", c, 0), xr.at[c, 0])
        recv(("xl", c, 0), xl.at[c, 0])
        recv(("xr", c, 1), xr.at[c, 1])
        for cols in thirds[:2]:
            zs[c, :, cols] = (
                part[k, piece(c, x, 1 - zl), cols].astype(F32)
                + xl[c, 1 - zl, :, cols].astype(F32)
                + xr[c, 1 - zl, :, cols].astype(F32)
            ).astype(BF16)
        send(("zz", c), zs.at[c], zr.at[c], zpeer)
        for cols in thirds[:2]:
            fo[c, :, cols] = (
                part[k, piece(c, x, zl), cols].astype(F32)
                + xl[c, zl, :, cols].astype(F32)
                + xr[c, zl, :, cols].astype(F32)
            )

    def sum3b(c):
        recv(("dm", c), dmid.at[c])
        if c % 2:
            add_to(piece(c, xm, zl), dh_cols, dmid[c])
            send(("dr", c), dh_part(piece(c, xm, zl)), dxr.at[c], left)
        else:
            add_to(piece(c, xp, zl), dh_cols, dmid[c])
            send(("dl", c), dh_part(piece(c, xp, zl)), dxl.at[c], right)

    def middle(c):
        recv(("zz", c), zr.at[c])
        recv(("dl", c), dxl.at[c])
        recv(("dr", c), dxr.at[c])
        r = piece(c, x, zl)

        @pl.loop(0, half // 128)
        def _(n):
            c0, c1, c2 = (at_rows(j * half + n * 128, 128, 128) for j in range(3))
            gate = fo[c, :, c0] + zr[c, :, c0].astype(F32)
            up = fo[c, :, c1] + zr[c, :, c1].astype(F32)
            dh = part[k, r, c2].astype(F32) + dxl[c, :, c0].astype(F32) + dxr[c, :, c0].astype(F32)
            sig = 1.0 / (1.0 + jnp.exp(-gate))
            act = gate * sig
            hid[k, r, c0] = (act * up).astype(BF16)
            hid[k, r, c1] = (dh * up * sig * (1.0 + gate * (1.0 - sig))).astype(BF16)
            hid[k, r, c2] = (dh * act).astype(BF16)

        full = hid.at[k, r]
        send("", full, full, right, sem(("gl", c)) + zl)
        sem(("gl", c, "b"))
        send("", full, full, left, sem(("gr", c)) + zl)
        sem(("gr", c, "b"))
        send(("gz", c), full, full, zpeer)

    def pass_on(name, r, cols, device, index=None):
        ref = hid.at[k, r, cols]
        send(name, ref, ref, device, index)

    def spread1(c):
        gl, gr = sem(("gl", c)), sem(("gr", c))
        other = piece(c, x, 1 - zl)
        recv(("gz", c), hid.at[k, other])
        pass_on("", other, gu_cols, right, gl + 1 - zl)
        pass_on("", other, gu_cols, left, gr + 1 - zl)

    def spread2a(c):
        gl, gr = sem(("gl", c)), sem(("gr", c))
        recv("", hid.at[k, piece(c, xm, zl)], gl + zl)
        recv("", hid.at[k, piece(c, xp, zl)], gr + zl)
        if c % 2:
            pass_on(("fd", c), piece(c, xp, zl), dh_cols, left)
        else:
            pass_on(("fd", c), piece(c, xm, zl), dh_cols, right)
        pass_on(("du", c, "m"), piece(c, xm, zl), dh_cols, zpeer)
        pass_on(("du", c, "p"), piece(c, xp, zl), dh_cols, zpeer)

    def spread2b(c):
        gl, gr = sem(("gl", c)), sem(("gr", c))
        recv("", hid.at[k, piece(c, xm, 1 - zl), gu_cols], gl + 1 - zl)
        recv("", hid.at[k, piece(c, xp, 1 - zl), gu_cols], gr + 1 - zl)
        pass_on(("fl", c), piece(c, xm, 0), gu_cols, right)
        pass_on(("fr", c), piece(c, xp, 1), gu_cols, left)
        if c in PIECES:
            to_core(c, 0, ((x, 0), (x, 1), (xm, zl), (xp, zl)))

    def to_core(c, base, places):
        for i, (xx, zz) in enumerate(places):
            ref = hid.at[k, piece(c, xx, zz)]
            send(("gc", c, base + i), ref, ref, core)

    def from_core(c, base, places):
        for i, (xx, zz) in enumerate(places):
            recv(("gc", c, base + i), hid.at[1 - k, piece(c, xx, zz)])

    def spread3(c):
        recv(("fd", c), hid.at[k, piece(c, x2, zl), dh_cols])
        pass_on(("du", c, "f"), piece(c, x2, zl), dh_cols, zpeer)

    def spread4(c):
        recv(("fl", c), hid.at[k, piece(c, x2, 0), gu_cols])
        recv(("fr", c), hid.at[k, piece(c, x2, 1), gu_cols])
        recv(("du", c, "m"), hid.at[k, piece(c, xm, 1 - zl), dh_cols])
        recv(("du", c, "p"), hid.at[k, piece(c, xp, 1 - zl), dh_cols])
        recv(("du", c, "f"), hid.at[k, piece(c, x2, 1 - zl), dh_cols])
        if c in PIECES:
            to_core(c, 4, ((xm, 1 - zl), (xp, 1 - zl), (x2, 0), (x2, 1)))
        else:
            send(("gc", c), hid.at[k, chunk(c)], hid.at[k, chunk(c)], core)

    def last_terms(c, q):
        here = chunk(c)
        c0 = at_rows(q * half, half, 128)
        return dot(hid[q, here, thirds[0]], wd[c0, :], 1, 0), (
            dot(hid[q, here, thirds[1]], wg[:, c0], 1, 1) + dot(hid[q, here, thirds[2]], wu[:, c0], 1, 1)
        )

    def last1(c):
        a, b = last_terms(c, k)
        acc[chunk(c), :feat] = a
        acc[chunk(c), feat:] = b

    def last2(c):
        if c in PIECES:
            from_core(c, 0, ((x, 0), (x, 1), (xm, zl), (xp, zl)))
            from_core(c, 4, ((xm, 1 - zl), (xp, 1 - zl), (x2, 0), (x2, 1)))
        else:
            recv(("gc", c), hid.at[1 - k, chunk(c)])
        here = chunk(c)
        a, b = last_terms(c, 1 - k)
        o[here, :feat] = (acc[here, :feat] + a).astype(BF16)
        o[here, feat:] = (acc[here, feat:] + b).astype(BF16)

    def out_rows(slot, rel, piece):
        base = NUMBER[slot, rel] * ROWS
        return slice(base + piece.start, base + piece.stop)

    sides = (slice(0, feat), slice(feat, 2 * feat))

    def send_out(name, slot, rel, piece, dst, device, h):
        send((*name, h), o.at[out_rows(slot, rel, piece), sides[h]], dst, device)

    def add_out(slot, rel, piece, other, h):
        r = out_rows(slot, rel, piece)
        o[r, sides[h]] = (o[r, sides[h]].astype(F32) + other.astype(F32)).astype(BF16)

    def out(slot, rel):
        for h in range(2):
            c = sides[h]
            if slot == 3:
                send_out(("ym", rel, "l"), 3, rel, lo, yml.at[rel, :, c], up_y, h)
                send_out(("ym", rel, "r"), 3, rel, hi, ymr.at[rel, :, c], dn_y, h)
            if slot == 1:
                send_out(("yl", rel, "h"), 1, rel, hi, yl.at[rel, hi, c], up_y, h)
            if slot == 2:
                send_out(("yr", rel, "l"), 2, rel, lo, yr.at[rel, lo, c], dn_y, h)

    def relay(slot, rel, h):
        c = sides[h]
        if slot == 1:
            recv(("ym", rel, "l", h), yml.at[rel, :, c])
            add_out(1, rel, lo, yml[rel, :, c], h)
            send_out(("yl", rel, "l"), 1, rel, lo, yl.at[rel, lo, c], up_y, h)
        else:
            recv(("ym", rel, "r", h), ymr.at[rel, :, c])
            add_out(2, rel, hi, ymr[rel, :, c], h)
            send_out(("yr", rel, "h"), 2, rel, hi, yr.at[rel, hi, c], dn_y, h)

    def gather_out(rel, h):
        c = sides[h]
        recv(("yl", rel, "h", h), yl.at[rel, hi, c])
        recv(("yr", rel, "l", h), yr.at[rel, lo, c])
        recv(("yl", rel, "l", h), yl.at[rel, lo, c])
        recv(("yr", rel, "h", h), yr.at[rel, hi, c])
        r = chunk(NUMBER[0, rel])
        return o[r, c].astype(F32) + yl[rel, :, c].astype(F32) + yr[rel, :, c].astype(F32)

    def finish1(h):
        yzs[:, sides[h]] = gather_out(1, h).astype(BF16)
        send(("yz", h), yzs.at[:, sides[h]], yzr.at[:, sides[h]], zhpeer)

    def finish0(h):
        total = gather_out(0, h)
        recv(("yz", h), yzr.at[:, sides[h]])
        both[:, sides[h]] = (total + yzr[:, sides[h]].astype(F32)).astype(BF16)

    rows_early = slice(0, EARLY * ROWS)

    def grad(i):
        if i < 4:
            q, m = i // 2, i % 2
            c = slice(q * half, (q + 1) * half)
            f = slice(m * feat // 2, (m + 1) * feat // 2)
            a = tc[rows_early, f]
            gg[f, c] = dot(a, hid[q, rows_early, thirds[1]], 0, 0).astype(BF16)
            gu[f, c] = dot(a, hid[q, rows_early, thirds[2]], 0, 0).astype(BF16)
        else:
            q = i - 4

            @pl.loop(0, half // 128)
            def _(n):
                h = hid[q, rows_early, at_rows(n * 128, 128, 128)]
                gd[at_rows(q * half + n * 128, 128, 128), :] = dot(
                    h, tc[rows_early, feat:], 0, 0
                ).astype(BF16)

    steps = (
        start, gather_a, gather_b, gather_b2, gather_c, first, second, sum1, sum1b, sum2a, sum2b, sum2c, sum3a, sum3b, middle, spread1, spread2a, spread2b, spread3, spread4, last1, last2, out, relay, finish1, finish0, grad,
    )
    for number, *arguments in ORDER:
        steps[number](*arguments)
    for copy in sent:
        copy.wait_send()


def finish(both, gg_in, gu_in, gd_in, hid, tc, out, gin, gg, gu, gd, bv, ga, ua, da, turned, out_sem):
    feat, ff = gg_in.shape
    half = ff // 2
    rows = slice(EARLY * ROWS, tc.shape[0])
    leaving = []

    def leave(src, dst):
        copy = pltpu.make_async_copy(src, dst, out_sem.at[len(leaving)])
        copy.start()
        leaving.append(copy)

    bv[...] = both[...]
    leave(bv.at[:, :feat], out)
    leave(bv.at[:, feat:], gin)
    turned[...] = tc[rows, :feat].T
    for third, before, total, dst in ((1, gg_in, ga, gg), (2, gu_in, ua, gu)):
        for f in (slice(n * TILE, (n + 1) * TILE) for n in range(feat // TILE)):
            for q in range(2):
                c = slice(q * half, (q + 1) * half)
                more = dot(turned[f], hid[q, rows, third * half : (third + 1) * half], 1, 0)
                total[f, c] = (before[f, c].astype(F32) + more).astype(BF16)
            leave(total.at[f], dst.at[f])
    step = 128
    for q in range(2):
        for n in range(half // step):
            u = slice(q * half + n * step, q * half + (n + 1) * step)
            more = dot(hid[q, rows, n * step : (n + 1) * step], tc[rows, feat:], 0, 0)
            da[u] = (gd_in[u].astype(F32) + more).astype(BF16)
            leave(da.at[u], gd.at[u])
    for copy in leaving:
        copy.wait()


def per_device(tokens, cotangent, gate_weight, up_weight, down_weight):
    feat, ff = gate_weight.shape
    half = ff // 2
    count = 8 * ROWS
    vmem = pl.BlockSpec(memory_space=pltpu.VMEM)
    hbm = pl.BlockSpec(memory_space=pl.ANY)
    shape = lambda *s: jax.ShapeDtypeStruct(s, BF16)
    buf = lambda *s: pltpu.VMEM(s, BF16)
    kept = pl.pallas_call(
        exchange,
        out_shape=(
            buf(ROWS, 2 * feat), buf(feat, ff), buf(feat, ff), buf(ff, feat),
            buf(2, count, 3 * half), buf(count, 2 * feat),
        ),
        in_specs=[hbm] * 5,
        out_specs=[vmem] * 6,
        scratch_shapes=[
            buf(feat, ff), buf(feat, ff), buf(ff, feat),
            buf(2, count, 3 * half), buf(8, ROWS, 3 * half),
            buf(8, 16, 2 * half), buf(8, 16, 2 * half),
            buf(8, 2, 16, 2 * half), buf(8, 2, 16, 2 * half),
            pltpu.VMEM((8, 16, 2 * half), F32), buf(8, 16, 2 * half), buf(8, 16, 2 * half),
            buf(8, 64, half), buf(8, 16, half), buf(8, 16, half), buf(8, 16, half),
            pltpu.VMEM((count, 2 * feat), F32), buf(count, 2 * feat),
            buf(2, 64, 2 * feat), buf(2, 64, 2 * feat),
            buf(2, ROWS, 2 * feat), buf(2, ROWS, 2 * feat),
            buf(ROWS, 2 * feat), buf(ROWS, 2 * feat),
            pltpu.SemaphoreType.DMA((320,)), pltpu.SemaphoreType.DMA((320,)), pltpu.SemaphoreType.DMA((8,)),
        ],
        compiler_params=pltpu.CompilerParams(
            collective_id=0, has_side_effects=True, vmem_limit_bytes=40 * 2**20
        ),
    )(tokens, cotangent, gate_weight, up_weight, down_weight)
    return pl.pallas_call(
        finish,
        out_shape=(shape(ROWS, feat), shape(ROWS, feat), shape(feat, ff), shape(feat, ff), shape(ff, feat)),
        in_specs=[vmem] * 6,
        out_specs=[hbm] * 5,
        scratch_shapes=[
            buf(ROWS, 2 * feat), buf(feat, ff), buf(feat, ff), buf(ff, feat),
            buf(feat, count - EARLY * ROWS),
            pltpu.SemaphoreType.DMA((2 * feat // TILE + ff // 128 + 2,)),
        ],
        compiler_params=pltpu.CompilerParams(vmem_limit_bytes=12 * 2**20),
    )(*kept)


def solution(mesh):
    placed = (P("mp", "dp"), P("mp", "dp"), P("dp", "mp"), P("dp", "mp"), P("mp", "dp"))
    return jax.shard_map(
        per_device, mesh=mesh, in_specs=placed, out_specs=placed, check_vma=False
    )
```
